256 devices in a mesh: row: 32 (over x, z_hi, core), col: 8 (over z_lo, y).
Axes of the slice: x: 4, y: 4, z: 8 (z_hi: 4, z_lo: 2; z = z_hi * 2 + z_lo), core: 2. Of those that a mesh axis runs over, the one named last changes fastest.
Arguments:
- amplitudes: float32 [32, 8, 1024, 1024], P('row', 'col'), may hold values from -6 to 6
- panels_left: bfloat16 [32, 2, 1024, 1024], P('row', None, 'col'), may hold values from -6 to 6
- panels_right: bfloat16 [8, 2, 1024, 1024], P('col', None, 'row'), may hold values from -6 to 6
- weights_right: bfloat16 [2, 8, 1024, 1024], P(None, 'col', 'row'), may hold values from -0.125 to 0.125
- weights_left: bfloat16 [2, 32, 1024, 1024], P(None, 'row', 'col'), may hold values from -0.125 to 0.125
- energy_left: float32 [32], P('row'), may hold values from -2 to -0.5
- energy_right: float32 [8], P('col'), may hold values from -2 to -0.5
- energy_virtual: float32 [1024], replicated, may hold values from 0.5 to 3
Outputs:
- updated: float32 [32, 8, 1024, 1024], P('row', 'col')
The draws below stay inside these ranges and needn't reach their ends.
All inputs are finite; a program needn't handle non-finite values.
Results may differ from the reference program's by a relative error of at most 0.0018.
Values may be sent and summed in bfloat16 or wider, within the bound.
A program may use at most 128 MiB of HBM per device.

```python
import jax
import jax.numpy as jnp
from jax import lax

VIRT = 1024
PANELS = 2
LEFT = 32
RIGHT = 8


def steps_of(own_key, shape, split, least, high):
    def one(position, shards_of):
        draws = jax.random.uniform(jax.random.fold_in(jax.random.fold_in(own_key, 6), position), (shards_of,), jnp.float32, least / len(split), high / len(split))
        return jnp.repeat(jnp.exp(draws), shape[position] // shards_of).reshape((-1,) + (1,) * (len(shape) - position - 1))

    level = one(*split[0])
    for cut in split[1:]:
        level = level * one(*cut)
    return level


def gaussian(own_key, extent, scale, bound, shards=(), kind=jnp.bfloat16):
    loudness = steps_of(own_key, extent, shards, -0.22, 0.18) if shards else 1.0
    values = jax.random.normal(own_key, extent, jnp.float32) * scale * loudness
    return jnp.minimum(jnp.maximum(values, -bound), bound).astype(kind)


def setup_inputs(seed: int = 0) -> dict:
    key_of = jax.random.split(jax.random.key(seed), 9)
    return {
        "amplitudes": gaussian(key_of[0], (LEFT, RIGHT, VIRT, VIRT), 1.0, 6.0, ((0, 32), (1, 8)), jnp.float32),
        "panels_left": gaussian(key_of[1], (LEFT, PANELS, VIRT, VIRT), 1.0, 6.0, ((0, 32), (2, 8))),
        "panels_right": gaussian(key_of[2], (RIGHT, PANELS, VIRT, VIRT), 1.0, 6.0, ((0, 8), (2, 32))),
        "weights_right": gaussian(key_of[3], (PANELS, RIGHT, VIRT, VIRT), (PANELS * VIRT) ** -0.5, 0.125, ((1, 8), (2, 32))),
        "weights_left": gaussian(key_of[4], (PANELS, LEFT, VIRT, VIRT), (PANELS * VIRT) ** -0.5, 0.125, ((1, 32), (2, 8))),
        "energy_left": jnp.clip(-2.0 + 1.5 * jax.random.uniform(key_of[5], (LEFT,), jnp.float32) ** steps_of(key_of[5], (LEFT,), ((0, 32),), -0.2, 0.2), -2.0, -0.5),
        "energy_right": jnp.clip(-2.0 + 1.5 * jax.random.uniform(key_of[6], (RIGHT,), jnp.float32) ** steps_of(key_of[6], (RIGHT,), ((0, 8),), -0.2, 0.2), -2.0, -0.5),
        "energy_virtual": jnp.clip(jax.random.uniform(key_of[7], (VIRT,), jnp.float32, 0.5, 3.0), 0.5, 3.0),
    }


def combine_blocks(blocks):
    as_float = blocks.astype(jnp.float32)
    return (2.0 * as_float - jnp.swapaxes(as_float, -1, -2)).astype(jnp.bfloat16)


def reference(amplitudes, panels_left, panels_right, weights_right, weights_left, energy_left, energy_right, energy_virtual):
    left_mixed = combine_blocks(panels_left).astype(jnp.float32)
    right_mixed = combine_blocks(panels_right).astype(jnp.float32)
    right_float = weights_right.astype(jnp.float32)
    left_float = weights_left.astype(jnp.float32)
    virt_pair = energy_virtual[:, None] + energy_virtual[None, :]

    def one_left(index):
        direct = jnp.einsum("kac,kjcb->jab", left_mixed[index], right_float)
        weight_here = lax.dynamic_index_in_dim(left_float, index, 1, keepdims=False)
        mirror = jnp.einsum("jkac,kcb->jab", right_mixed, weight_here)
        residual = direct + jnp.swapaxes(mirror, 1, 2)
        denominator = energy_left[index] + energy_right[:, None, None] - virt_pair[None, :, :]
        return amplitudes[index] + residual / denominator

    return lax.map(one_left, jnp.arange(amplitudes.shape[0], dtype=jnp.int32))
```

```python
import jax
import jax.numpy as jnp
from jax import lax
from jax.experimental import pallas as pl
from jax.experimental.pallas import tpu as pltpu
from jax.sharding import PartitionSpec as P

MESH = pl.DeviceIdType.MESH
F32 = jnp.float32
BF16 = jnp.bfloat16
N_MSG = 64


def gather_kernel(panl, panr, wtr, wtl, out, awi, awj, lm, rmt, wt, lsem, ssem, rsem):
    row, col = lax.axis_index("row"), lax.axis_index("col")
    x, zh, core = row // 8, lax.rem(row // 2, 4), lax.rem(row, 2)
    zl, y = col // 4, lax.rem(col, 4)

    def at_x(d):
        return lax.rem(x + d + 4, 4)

    def at_z(d):
        return lax.rem(zh + d + 4, 4)

    def at_y(d):
        return lax.rem(y + d + 4, 4)

    def row_of(x_, zh_, core_):
        return (x_ * 4 + zh_) * 2 + core_

    dev = {
        "x+": (row_of(at_x(1), zh, core), col),
        "x-": (row_of(at_x(-1), zh, core), col),
        "z+": (row_of(x, at_z(1), core), col),
        "z-": (row_of(x, at_z(-1), core), col),
        "y+": (row, zl * 4 + at_y(1)),
        "y-": (row, zl * 4 + at_y(-1)),
        "zi": (row, (1 - zl) * 4 + y),
        "core": (row_of(x, zh, 1 - core), col),
    }

    own = [
        pltpu.make_async_copy(panl, awi.at[0:2, col], lsem.at[0]),
        pltpu.make_async_copy(panr, awj.at[0:2, x, zh, core], lsem.at[1]),
        pltpu.make_async_copy(wtr, awj.at[2:4, x, zh, core], lsem.at[2]),
        pltpu.make_async_copy(wtl, awi.at[2:4, col], lsem.at[3]),
    ]
    for copy in own:
        copy.start()

    barrier = pltpu.get_barrier_semaphore()
    for peer in dev.values():
        pl.semaphore_signal(barrier, inc=1, device_id=peer, device_id_type=MESH)
    pl.semaphore_wait(barrier, len(dev))
    for copy in own:
        copy.wait()

    ids = {}
    sent = []

    def describe(name, ref, to):
        number = ids.setdefault(name, len(ids))
        return pltpu.make_async_remote_copy(
            src_ref=ref, dst_ref=ref, send_sem=ssem.at[number], recv_sem=rsem.at[number],
            device_id=dev[to], device_id_type=MESH,
        )

    def send(name, ref, to):
        copy = describe(name, ref, to)
        copy.start()
        sent.append(copy)

    def got(name, ref):
        describe(name, ref, "core").wait_recv()

    def j(dx, dz, lo=0, hi=4):
        return awj.at[lo:hi, at_x(dx), at_z(dz), core]

    def i(part, dy, same=True, lo=0, hi=128):
        return awi.at[part, (zl if same else 1 - zl) * 4 + at_y(dy), lo:hi]

    A0, A1, W0, W1 = 0, 1, 2, 3
    OPP = {"+": "-", "-": "+"}
    STEP = {"+": 1, "-": -1}

    def ring_send(tag, part, same, signs="+-"):
        for s in signs:
            send(f"{tag}{part}{s}", i(part, 0, same), "y" + s)

    def ring_got(tag, part, same, s):
        got(f"{tag}{part}{s}", i(part, -STEP[s], same))

    def ring_forward(tag, part, same, s, lo=0, hi=128):
        send(f"{tag}f{part}{s}", i(part, -STEP[s], same, lo, hi), "y" + s)

    def ring_got_forward(tag, part, same, s, lo=0, hi=128):
        got(f"{tag}f{part}{s}", i(part, 2, same, lo, hi))

    def x_send(dz):
        for s in "+-":
            send(f"x{dz}{s}", j(0, dz), "x" + s)

    def x_forward(dz):
        for s in "+-":
            got(f"x{dz}{s}", j(-STEP[s], dz))
        send(f"xf{dz}+", j(-1, dz, 0, 2), "x+")
        send(f"xf{dz}-", j(1, dz, 2, 4), "x-")

    def x_got_forward(dz):
        got(f"xf{dz}+", j(2, dz, 0, 2))
        got(f"xf{dz}-", j(2, dz, 2, 4))

    def share(dx):
        send(f"core{dx}", awj.at[:, at_x(dx), :, core], "core")

    def got_share(dx):
        got(f"core{dx}", awj.at[:, at_x(dx), :, 1 - core])

    def mix_left(blk):
        start = pl.multiple_of(blk * 128, 128)

        def one(k, _):
            for h in range(2):
                cols = slice(h * 512, h * 512 + 512)
                straight = awi[k, blk, :, cols].astype(F32)
                turned = awi[k, h * 4:h * 4 + 4, :, pl.ds(start, 128)].reshape(512, 128).T.astype(F32)
                lm[k, pl.ds(start, 128), cols] = (2.0 * straight - turned).astype(BF16)
            return _

        lax.fori_loop(0, 2, one, 0)

    def mix_right(blk):
        start = pl.multiple_of(blk * 128, 128)

        def one(k, _):
            for h in range(2):
                cols = slice(h * 512, h * 512 + 512)
                straight = awj[k, blk // 2, pl.ds(lax.rem(blk, 2) * 2, 2), :, :, cols].reshape(128, 512).astype(F32)
                turned = awj[k, h * 2:h * 2 + 2, :, :, :, pl.ds(start, 128)].reshape(512, 128).T.astype(F32)
                rmt[blk, pl.ds(pl.multiple_of(k * 128, 128), 128), cols] = (2.0 * turned - straight).astype(BF16)
            return _

        lax.fori_loop(0, 2, one, 0)

    def direct_tile(m):
        rows = pl.ds(pl.multiple_of(m * 256, 256), 256)

        def one(n, _):
            cols = pl.ds(pl.multiple_of(n * 256, 256), 256)
            total = jnp.zeros((256, 256), F32)
            for k in range(2):
                total += jnp.dot(lm[k, rows, :], awj[2 + k, :, :, :, :, cols].reshape(1024, 256),
                                 preferred_element_type=F32)
            out[rows, cols] = total
            return _

        lax.fori_loop(0, 4, one, 0)

    def mirror_slot(slot):
        for k in range(2):
            for h in range(2):
                cols = slice(h * 512, h * 512 + 512)
                wt[cols, k * 128:k * 128 + 128] = awi[2 + k, slot, :, cols].T

        def one(n, _):
            cols = pl.ds(pl.multiple_of(n * 256, 256), 256)
            out[:, cols] += jnp.dot(wt[...], rmt[slot, :, cols], preferred_element_type=F32)
            return _

        lax.fori_loop(0, 4, one, 0)

    def loop(count, task):
        def one(n, _):
            task(n)
            return _
        lax.fori_loop(0, count, one, 0)

    def slot_of(dy, same):
        return (zl if same else 1 - zl) * 4 + at_y(dy)

    send("jz+", j(0, 0), "z+")
    send("jz-", j(0, 0), "z-")
    ring_send("y", A0, True)
    ring_send("y", A1, True)
    x_send(0)
    send("zA0", i(A0, 0), "zi")
    send("zA1", i(A1, 0), "zi")
    ring_send("y", W1, True)
    send("zW0", i(W0, 0), "zi")
    send("zW1.0", i(W1, 0), "zi")

    x_forward(0)
    got("jz+", j(0, -1))
    got("jz-", j(0, 1))
    send("jzf+", j(0, -1, 0, 2), "z+")
    send("jzf-", j(0, 1, 2, 4), "z-")
    x_send(-1)
    x_send(1)
    ring_got("y", A0, True, "+")
    ring_forward("y", A0, True, "+")
    ring_got("y", A1, True, "-")
    ring_forward("y", A1, True, "-")
    got("zA0", i(A0, 0, False))
    ring_send("p", A0, False)
    got("zA1", i(A1, 0, False))
    ring_send("p", A1, False)
    got("jzf+", j(0, 2, 0, 2))
    got("jzf-", j(0, 2, 2, 4))
    x_send(2)
    share(0)
    x_got_forward(0)
    x_forward(-1)
    x_forward(1)
    ring_got("y", W1, True, "+")
    ring_got("y", W1, True, "-")
    send("zW1.-", i(W1, -1), "zi")
    send("zW1.+", i(W1, 1), "zi")
    ring_got("y", A0, True, "-")
    ring_got("y", A1, True, "+")
    ring_got_forward("y", A0, True, "+")
    ring_got_forward("y", A1, True, "-")
    ring_got("p", A0, False, "+")
    ring_forward("p", A0, False, "+")
    ring_got("p", A1, False, "-")
    ring_forward("p", A1, False, "-")
    ring_forward("y", W1, True, "+", 0, 64)
    ring_forward("y", W1, True, "-", 64, 128)
    ring_send("y", W0, True)
    got("zW0", i(W0, 0, False))
    ring_send("p", W0, False)
    x_forward(2)
    x_got_forward(-1)
    x_got_forward(1)
    x_got_forward(2)
    for dx in (-1, 1, 2):
        share(dx)
    ring_got_forward("y", W1, True, "+", 0, 64)
    ring_got_forward("y", W1, True, "-", 64, 128)
    send("zW1.2", i(W1, 2), "zi")
    ring_got("p", A0, False, "-")
    ring_got("p", A1, False, "+")
    ring_got_forward("p", A0, False, "+")
    ring_got_forward("p", A1, False, "-")
    loop(8, mix_left)
    for dx in (0, -1, 1, 2):
        got_share(dx)
    loop(8, mix_right)
    ring_got("y", W0, True, "+")
    ring_got("y", W0, True, "-")
    ring_forward("y", W0, True, "+", 0, 64)
    ring_forward("y", W0, True, "-", 64, 128)
    loop(4, direct_tile)
    mirror_slot(slot_of(0, True))
    ring_got("p", W0, False, "+")
    ring_got("p", W0, False, "-")
    ring_forward("p", W0, False, "+", 0, 64)
    ring_forward("p", W0, False, "-", 64, 128)
    mirror_slot(slot_of(-1, True))
    mirror_slot(slot_of(1, True))
    got("zW1.0", i(W1, 0, False))
    mirror_slot(slot_of(0, False))
    got("zW1.-", i(W1, -1, False))
    mirror_slot(slot_of(-1, False))
    got("zW1.+", i(W1, 1, False))
    mirror_slot(slot_of(1, False))
    ring_got_forward("y", W0, True, "+", 0, 64)
    ring_got_forward("y", W0, True, "-", 64, 128)
    mirror_slot(slot_of(2, True))
    got("zW1.2", i(W1, 2, False))
    ring_got_forward("p", W0, False, "+", 0, 64)
    ring_got_forward("p", W0, False, "-", 64, 128)
    mirror_slot(slot_of(2, False))
    for copy in sent:
        copy.wait_send()
    assert len(ids) <= N_MSG


def body(amplitudes, panels_left, panels_right, weights_right, weights_left, energy_left, energy_right, energy_virtual):
    residual = pl.pallas_call(
        gather_kernel,
        out_shape=jax.ShapeDtypeStruct((1024, 1024), F32),
        in_specs=[pl.BlockSpec(memory_space=pl.ANY)] * 4,
        out_specs=pl.BlockSpec(memory_space=pltpu.VMEM),
        scratch_shapes=[
            pltpu.VMEM((4, 8, 128, 1024), BF16),
            pltpu.VMEM((4, 4, 4, 2, 32, 1024), BF16),
            pltpu.VMEM((2, 1024, 1024), BF16),
            pltpu.VMEM((8, 256, 1024), BF16),
            pltpu.VMEM((1024, 256), BF16),
            pltpu.SemaphoreType.DMA((4,)),
            pltpu.SemaphoreType.DMA((N_MSG,)),
            pltpu.SemaphoreType.DMA((N_MSG,)),
        ],
        compiler_params=pltpu.CompilerParams(
            collective_id=0, has_side_effects=True, vmem_limit_bytes=44 * 1024 * 1024
        ),
        name="gather_products",
    )(panels_left[0], panels_right[0], weights_right[:, 0], weights_left[:, 0])
    virt_pair = energy_virtual[:, None] + energy_virtual[None, :]
    denominator = energy_left[0] + energy_right[0] - virt_pair
    return (amplitudes[0, 0] + residual / denominator)[None, None]


def solution(mesh):
    placed = (
        P("row", "col", None, None),
        P("row", None, "col", None),
        P("col", None, "row", None),
        P(None, "col", "row", None),
        P(None, "row", "col", None),
        P("row"),
        P("col"),
        P(),
    )
    return jax.shard_map(
        body, mesh=mesh, in_specs=placed, out_specs=P("row", "col", None, None), check_vma=False
    )
```

```python
import jax
import jax.numpy as jnp
from jax import lax
from jax.experimental import pallas as pl
from jax.experimental.pallas import tpu as pltpu
from jax.sharding import PartitionSpec as P

MESH = pl.DeviceIdType.MESH
F32 = jnp.float32
BF16 = jnp.bfloat16
N_MSG = 56


def gather_kernel(panl, panr, wtr, wtl, amp_in, ev_in, el, er, out, awi, awj, lm, rmt, wt, amp, inv, ev,
                  lsem, ssem, rsem):
    row, col = lax.axis_index("row"), lax.axis_index("col")
    x, zh, core = row // 8, lax.rem(row // 2, 4), lax.rem(row, 2)
    zl, y = col // 4, lax.rem(col, 4)

    def at_x(d):
        return lax.rem(x + d + 4, 4)

    def at_z(d):
        return lax.rem(zh + d + 4, 4)

    def at_y(d):
        return lax.rem(y + d + 4, 4)

    def row_of(x_, zh_, core_):
        return (x_ * 4 + zh_) * 2 + core_

    dev = {
        "x+": (row_of(at_x(1), zh, core), col),
        "x-": (row_of(at_x(-1), zh, core), col),
        "z+": (row_of(x, at_z(1), core), col),
        "z-": (row_of(x, at_z(-1), core), col),
        "y+": (row, zl * 4 + at_y(1)),
        "y-": (row, zl * 4 + at_y(-1)),
        "zi": (row, (1 - zl) * 4 + y),
        "core": (row_of(x, zh, 1 - core), col),
    }

    own = [
        pltpu.make_async_copy(panl, awi.at[0:2, col], lsem.at[0]),
        pltpu.make_async_copy(panr, awj.at[0:2, x, zh, core], lsem.at[1]),
        pltpu.make_async_copy(wtr, awj.at[2:4, x, zh, core], lsem.at[2]),
        pltpu.make_async_copy(wtl, awi.at[2:4, col], lsem.at[3]),
    ]
    small = [
        pltpu.make_async_copy(ev_in, ev, lsem.at[4]),
    ]
    load = pltpu.make_async_copy(amp_in, amp, lsem.at[5])
    for copy in own + small + [load]:
        copy.start()

    barrier = pltpu.get_barrier_semaphore()
    for peer in dev.values():
        pl.semaphore_signal(barrier, inc=1, device_id=peer, device_id_type=MESH)
    pl.semaphore_wait(barrier, len(dev))
    for copy in own:
        copy.wait()

    ids = {}
    sent = []

    def describe(name, ref, to):
        number = ids.setdefault(name, len(ids))
        return pltpu.make_async_remote_copy(
            src_ref=ref, dst_ref=ref, send_sem=ssem.at[number], recv_sem=rsem.at[number],
            device_id=dev[to], device_id_type=MESH,
        )

    def send(name, ref, to):
        copy = describe(name, ref, to)
        copy.start()
        sent.append(copy)

    def got(name, ref):
        describe(name, ref, "core").wait_recv()

    def j(dx, dz, lo=0, hi=4):
        return awj.at[lo:hi, at_x(dx), at_z(dz), core]

    def i(part, dy, same=True, lo=0, hi=128):
        return awi.at[part, (zl if same else 1 - zl) * 4 + at_y(dy), lo:hi]

    A0, A1, W0, W1 = 0, 1, 2, 3
    OPP = {"+": "-", "-": "+"}
    STEP = {"+": 1, "-": -1}

    def ring_send(tag, part, same, signs="+-"):
        for s in signs:
            send(f"{tag}{part}{s}", i(part, 0, same), "y" + s)

    def ring_got(tag, part, same, s):
        got(f"{tag}{part}{s}", i(part, -STEP[s], same))

    def ring_forward(tag, part, same, s, lo=0, hi=128):
        send(f"{tag}f{part}{s}", i(part, -STEP[s], same, lo, hi), "y" + s)

    def ring_got_forward(tag, part, same, s, lo=0, hi=128):
        got(f"{tag}f{part}{s}", i(part, 2, same, lo, hi))

    def x_send(dz):
        for s in "+-":
            send(f"x{dz}{s}", j(0, dz), "x" + s)

    def x_forward(dz):
        for s in "+-":
            got(f"x{dz}{s}", j(-STEP[s], dz))
        send(f"xf{dz}+", j(-1, dz, 0, 2), "x+")
        send(f"xf{dz}-", j(1, dz, 2, 4), "x-")

    def x_got_forward(dz):
        got(f"xf{dz}+", j(2, dz, 0, 2))
        got(f"xf{dz}-", j(2, dz, 2, 4))

    def share(dx):
        send(f"core{dx}", awj.at[:, at_x(dx), :, core], "core")

    def got_share(dx):
        got(f"core{dx}", awj.at[:, at_x(dx), :, 1 - core])

    def mix_left(blk):
        start = pl.multiple_of(blk * 128, 128)

        def one(k, _):
            for h in range(2):
                cols = slice(h * 512, h * 512 + 512)
                straight = awi[k, blk, :, cols].astype(F32)
                turned = awi[k, h * 4:h * 4 + 4, :, pl.ds(start, 128)].reshape(512, 128).T.astype(F32)
                lm[k, pl.ds(start, 128), cols] = (2.0 * straight - turned).astype(BF16)
            return _

        lax.fori_loop(0, 2, one, 0)

    def mix_right(blk):
        start = pl.multiple_of(blk * 128, 128)

        def one(k, _):
            for h in range(2):
                cols = slice(h * 512, h * 512 + 512)
                straight = awj[k, blk // 2, pl.ds(lax.rem(blk, 2) * 2, 2), :, :, cols].reshape(128, 512).astype(F32)
                turned = awj[k, h * 2:h * 2 + 2, :, :, :, pl.ds(start, 128)].reshape(512, 128).T.astype(F32)
                rmt[blk, pl.ds(pl.multiple_of(k * 128, 128), 128), cols] = (2.0 * turned - straight).astype(BF16)
            return _

        lax.fori_loop(0, 2, one, 0)

    def direct_tile(m):
        rows = pl.ds(pl.multiple_of(m * 256, 256), 256)

        def one(n, _):
            cols = pl.ds(pl.multiple_of(n * 256, 256), 256)
            total = jnp.zeros((256, 256), F32)
            for k in range(2):
                total += jnp.dot(lm[k, rows, :], awj[2 + k, :, :, :, :, cols].reshape(1024, 256),
                                 preferred_element_type=F32)
            out[rows, cols] = total
            return _

        lax.fori_loop(0, 4, one, 0)

    def mirror_slots(places, last=False):
        slots = [slot_of(*place) for place in places]
        for p, slot in enumerate(slots):
            for k in range(2):
                for h in range(2):
                    cols = slice(h * 512, h * 512 + 512)
                    start = (2 * p + k) * 128
                    wt[cols, start:start + 128] = awi[2 + k, slot, :, cols].T

        def one(n, _):
            cols = pl.ds(pl.multiple_of(n * 256, 256), 256)
            total = out[:, cols]
            for p, slot in enumerate(slots):
                total += jnp.dot(wt[:, p * 256:p * 256 + 256], rmt[slot, :, cols], preferred_element_type=F32)
            out[:, cols] = amp[:, cols] + total * inv[:, cols] if last else total
            return _

        lax.fori_loop(0, 4, one, 0)

    def inverse_rows(blk):
        pair = el[0] + er[0]
        turned = jnp.broadcast_to(ev[pl.ds(blk, 1), :], (128, 128)).T
        for q in range(8):
            virt_pair = turned + ev[q:q + 1, :]
            inv[pl.ds(pl.multiple_of(blk * 128, 128), 128), q * 128:q * 128 + 128] = 1.0 / (pair - virt_pair)

    def loop(count, task):
        def one(n, _):
            task(n)
            return _
        lax.fori_loop(0, count, one, 0)

    def slot_of(dy, same):
        return (zl if same else 1 - zl) * 4 + at_y(dy)

    send("jz+", j(0, 0), "z+")
    send("jz-", j(0, 0), "z-")
    ring_send("y", A0, True)
    ring_send("y", A1, True)
    x_send(0)
    send("zA0", i(A0, 0), "zi")
    ring_send("y", W1, True)
    for copy in small:
        copy.wait()
    loop(2, inverse_rows)

    x_forward(0)
    ring_got("y", A0, True, "+")
    ring_forward("y", A0, True, "+")
    got("jz+", j(0, -1))
    got("jz-", j(0, 1))
    send("jzf+", j(0, -1, 0, 2), "z+")
    send("jzf-", j(0, 1, 2, 4), "z-")
    x_send(-1)
    x_send(1)
    send("zA1", i(A1, 0), "zi")
    send("zW0", i(W0, 0), "zi")
    send("zW1.0", i(W1, 0), "zi")
    ring_got("y", A1, True, "-")
    ring_forward("y", A1, True, "-")
    loop(2, lambda n: inverse_rows(n + 2))
    got("zA0", i(A0, 0, False))
    ring_send("p", A0, False)
    ring_got("y", W1, True, "+")
    ring_got("y", W1, True, "-")
    send("zW1.-", i(W1, -1), "zi")
    send("zW1.+", i(W1, 1), "zi")
    ring_forward("y", W1, True, "+", 0, 64)
    ring_forward("y", W1, True, "-", 64, 128)
    loop(2, lambda n: inverse_rows(n + 4))
    got("jzf+", j(0, 2, 0, 2))
    got("jzf-", j(0, 2, 2, 4))
    x_send(2)
    x_forward(-1)
    x_forward(1)
    x_got_forward(0)
    share(0)
    loop(2, lambda n: inverse_rows(n + 6))
    got("zA1", i(A1, 0, False))
    ring_send("p", A1, False)
    ring_got("p", A0, False, "+")
    ring_forward("p", A0, False, "+")
    x_forward(2)
    ring_got_forward("y", W1, True, "+", 0, 64)
    ring_got_forward("y", W1, True, "-", 64, 128)
    send("zW1.2", i(W1, 2), "zi")
    ring_got("p", A1, False, "-")
    ring_forward("p", A1, False, "-")
    ring_send("y", W0, True)
    got("zW0", i(W0, 0, False))
    ring_send("p", W0, False)
    x_got_forward(-1)
    x_got_forward(1)
    for dx in (-1, 1):
        share(dx)
    x_got_forward(2)
    share(2)
    for dx in (0, -1, 1, 2):
        got_share(dx)
    loop(8, mix_right)
    ring_got("y", A0, True, "-")
    ring_got("y", A1, True, "+")
    ring_got_forward("y", A0, True, "+")
    ring_got_forward("y", A1, True, "-")
    ring_got("p", A0, False, "-")
    ring_got("p", A1, False, "+")
    ring_got_forward("p", A0, False, "+")
    ring_got_forward("p", A1, False, "-")
    loop(8, mix_left)
    direct_tile(0)
    ring_got("y", W0, True, "+")
    ring_got("y", W0, True, "-")
    ring_forward("y", W0, True, "+", 0, 64)
    ring_forward("y", W0, True, "-", 64, 128)
    loop(3, lambda n: direct_tile(n + 1))
    ring_got("p", W0, False, "+")
    ring_got("p", W0, False, "-")
    ring_forward("p", W0, False, "+", 0, 64)
    ring_forward("p", W0, False, "-", 64, 128)
    got("zW1.0", i(W1, 0, False))
    mirror_slots([(0, True), (0, False)])
    mirror_slots([(-1, True), (1, True)])
    got("zW1.-", i(W1, -1, False))
    got("zW1.+", i(W1, 1, False))
    mirror_slots([(-1, False), (1, False)])
    load.wait()
    ring_got_forward("y", W0, True, "+", 0, 64)
    ring_got_forward("y", W0, True, "-", 64, 128)
    got("zW1.2", i(W1, 2, False))
    ring_got_forward("p", W0, False, "+", 0, 64)
    ring_got_forward("p", W0, False, "-", 64, 128)
    mirror_slots([(2, True), (2, False)], True)
    for copy in sent:
        copy.wait_send()
    assert len(ids) <= N_MSG


def body(amplitudes, panels_left, panels_right, weights_right, weights_left, energy_left, energy_right, energy_virtual):
    updated = pl.pallas_call(
        gather_kernel,
        out_shape=jax.ShapeDtypeStruct((1024, 1024), F32),
        in_specs=[pl.BlockSpec(memory_space=pltpu.HBM)] * 6 + [pl.BlockSpec(memory_space=pltpu.SMEM)] * 2,
        out_specs=pl.BlockSpec(memory_space=pltpu.VMEM),
        scratch_shapes=[
            pltpu.VMEM((4, 8, 128, 1024), BF16),
            pltpu.VMEM((4, 4, 4, 2, 32, 1024), BF16),
            pltpu.VMEM((2, 1024, 1024), BF16),
            pltpu.VMEM((8, 256, 1024), BF16),
            pltpu.VMEM((1024, 512), BF16),
            pltpu.VMEM((1024, 1024), F32),
            pltpu.VMEM((1024, 1024), F32),
            pltpu.VMEM((8, 128), F32),
            pltpu.SemaphoreType.DMA((6,)),
            pltpu.SemaphoreType.DMA((N_MSG,)),
            pltpu.SemaphoreType.DMA((N_MSG,)),
        ],
        compiler_params=pltpu.CompilerParams(
            collective_id=0, has_side_effects=True, vmem_limit_bytes=48 * 1024 * 1024
        ),
        name="gather_products",
    )(*(pltpu.with_memory_space_constraint(array, pltpu.HBM) for array in (
        panels_left[0], panels_right[0], weights_right[:, 0], weights_left[:, 0], amplitudes[0, 0],
        energy_virtual.reshape(8, 128))), energy_left, energy_right)
    return updated[None, None]


def solution(mesh):
    placed = (
        P("row", "col", None, None),
        P("row", None, "col", None),
        P("col", None, "row", None),
        P(None, "col", "row", None),
        P(None, "row", "col", None),
        P("row"),
        P("col"),
        P(),
    )
    return jax.shard_map(
        body, mesh=mesh, in_specs=placed, out_specs=P("row", "col", None, None), check_vma=False
    )
```

```python
import jax
import jax.numpy as jnp
from jax import lax
from jax.experimental import pallas as pl
from jax.experimental.pallas import tpu as pltpu
from jax.sharding import PartitionSpec as P

MESH = pl.DeviceIdType.MESH
F32 = jnp.float32
BF16 = jnp.bfloat16
N_MSG = 56
CUT = 112


def gather_kernel(panl, panr, wtr, wtl, amp_in, ev_in, el, er, out, inv, wt, rmt, awi, awj, lm, amp, ev,
                  lsem, ssem, rsem):
    row, col = lax.axis_index("row"), lax.axis_index("col")
    x, zh, core = row // 8, lax.rem(row // 2, 4), lax.rem(row, 2)
    zl, y = col // 4, lax.rem(col, 4)

    def at_x(d):
        return lax.rem(x + d + 4, 4)

    def at_z(d):
        return lax.rem(zh + d + 4, 4)

    def at_y(d):
        return lax.rem(y + d + 4, 4)

    def row_of(x_, zh_, core_):
        return (x_ * 4 + zh_) * 2 + core_

    dev = {
        "x+": (row_of(at_x(1), zh, core), col),
        "x-": (row_of(at_x(-1), zh, core), col),
        "z+": (row_of(x, at_z(1), core), col),
        "z-": (row_of(x, at_z(-1), core), col),
        "y+": (row, zl * 4 + at_y(1)),
        "y-": (row, zl * 4 + at_y(-1)),
        "zi": (row, (1 - zl) * 4 + y),
        "core": (row_of(x, zh, 1 - core), col),
    }

    own = [
        pltpu.make_async_copy(panl, awi.at[col, 0:256], lsem.at[0]),
        pltpu.make_async_copy(panr, awj.at[0:2, x, zh, core], lsem.at[1]),
        pltpu.make_async_copy(wtr, awj.at[2:4, x, zh, core], lsem.at[2]),
        pltpu.make_async_copy(wtl, awi.at[col, 256:512], lsem.at[3]),
    ]
    small = [
        pltpu.make_async_copy(ev_in, ev, lsem.at[4]),
    ]
    load = pltpu.make_async_copy(amp_in, amp, lsem.at[5])
    for copy in own + small + [load]:
        copy.start()

    barrier = pltpu.get_barrier_semaphore()
    for peer in dev.values():
        pl.semaphore_signal(barrier, inc=1, device_id=peer, device_id_type=MESH)
    pl.semaphore_wait(barrier, len(dev))
    for copy in own:
        copy.wait()

    ids = {}
    sent = []

    def describe(name, ref, to):
        number = ids.setdefault(name, len(ids))
        return pltpu.make_async_remote_copy(
            src_ref=ref, dst_ref=ref, send_sem=ssem.at[number], recv_sem=rsem.at[number],
            device_id=dev[to], device_id_type=MESH,
        )

    def send(name, ref, to):
        copy = describe(name, ref, to)
        copy.start()
        sent.append(copy)

    def got(name, ref):
        describe(name, ref, "core").wait_recv()

    def j(dx, dz, lo=0, hi=4):
        return awj.at[lo:hi, at_x(dx), at_z(dz), core]

    def i(part, dy, same=True):
        return awi.at[(zl if same else 1 - zl) * 4 + at_y(dy), part[0]:part[1]]

    A0, A1, U, V = (0, 128), (128, 256), (256, 256 + CUT), (256 + CUT, 512)
    UP = {"+": (256, 320), "-": (320, 256 + CUT)}
    VP = {"+": (256 + CUT, 320 + CUT), "-": (320 + CUT, 512)}
    STEP = {"+": 1, "-": -1}

    def ring_send(tag, part, same):
        for s in "+-":
            send(f"{tag}{part}{s}", i(part, 0, same), "y" + s)

    def ring_got(tag, part, same, s):
        got(f"{tag}{part}{s}", i(part, -STEP[s], same))

    def ring_forward(tag, part, same, s):
        send(f"{tag}f{part}{s}", i(part, -STEP[s], same), "y" + s)

    def ring_got_forward(tag, part, same, s):
        got(f"{tag}f{part}{s}", i(part, 2, same))

    def x_send(dz):
        for s in "+-":
            send(f"x{dz}{s}", j(0, dz), "x" + s)

    def x_forward(dz):
        for s in "+-":
            got(f"x{dz}{s}", j(-STEP[s], dz))
        send(f"xf{dz}+", j(-1, dz, 0, 2), "x+")
        send(f"xf{dz}-", j(1, dz, 2, 4), "x-")

    def x_got_forward(dz):
        got(f"xf{dz}+", j(2, dz, 0, 2))
        got(f"xf{dz}-", j(2, dz, 2, 4))

    def share(dx):
        send(f"core{dx}", awj.at[:, at_x(dx), :, core], "core")

    def got_share(dx):
        got(f"core{dx}", awj.at[:, at_x(dx), :, 1 - core])

    def mix_left(blk):
        start = pl.multiple_of(blk * 128, 128)

        def one(k, _):
            own_rows = pl.ds(pl.multiple_of(k * 128, 128), 128)
            for h in range(2):
                cols = slice(h * 512, h * 512 + 512)
                straight = awi[blk, own_rows, cols].astype(F32)
                turned = awi[h * 4:h * 4 + 4, own_rows, pl.ds(start, 128)].reshape(512, 128).T.astype(F32)
                lm[k, pl.ds(start, 128), cols] = (2.0 * straight - turned).astype(BF16)
            return _

        lax.fori_loop(0, 2, one, 0)

    def mix_right(blk):
        start = pl.multiple_of(blk * 128, 128)

        def one(k, _):
            for h in range(2):
                cols = slice(h * 512, h * 512 + 512)
                straight = awj[k, blk // 2, pl.ds(lax.rem(blk, 2) * 2, 2), :, :, cols].reshape(128, 512).astype(F32)
                turned = awj[k, h * 2:h * 2 + 2, :, :, :, pl.ds(start, 128)].reshape(512, 128).T.astype(F32)
                rmt[blk, pl.ds(pl.multiple_of(k * 128, 128), 128), cols] = (2.0 * turned - straight).astype(BF16)
            return _

        lax.fori_loop(0, 2, one, 0)

    def direct_tile(n):
        cols = pl.ds(pl.multiple_of(n * 512, 512), 512)
        total = jnp.dot(lm[0], awj[2, :, :, :, :, cols].reshape(1024, 512), preferred_element_type=F32)
        total += jnp.dot(lm[1], awj[3, :, :, :, :, cols].reshape(1024, 512), preferred_element_type=F32)
        out[:, cols] += total

    def turn(p, slot):
        for k in range(2):
            for h in range(2):
                cols = slice(h * 512, h * 512 + 512)
                start = (2 * p + k) * 128
                wt[cols, start:start + 128] = awi[slot, 256 + k * 128:384 + k * 128, cols].T

    def mirror_slots(places, first=False, last=False):
        slots = [slot_of(*place) for place in places]
        for p, slot in enumerate(slots):
            turn(p, slot)

        def one(n, _):
            cols = pl.ds(pl.multiple_of(n * 512, 512), 512)
            total = jnp.zeros((1024, 512), F32) if first else out[:, cols]
            for p, slot in enumerate(slots):
                total += jnp.dot(wt[:, p * 256:p * 256 + 256], rmt[slot, :, cols], preferred_element_type=F32)
            out[:, cols] = amp[:, cols] + total * inv[:, cols] if last else total
            return _

        lax.fori_loop(0, 2, one, 0)

    def inverse_rows(blk):
        pair = el[0] + er[0]
        turned = jnp.broadcast_to(ev[pl.ds(blk, 1), :], (128, 128)).T
        for q in range(8):
            virt_pair = turned + ev[q:q + 1, :]
            inv[pl.ds(pl.multiple_of(blk * 128, 128), 128), q * 128:q * 128 + 128] = 1.0 / (pair - virt_pair)

    def loop(count, task):
        def one(n, _):
            task(n)
            return _
        lax.fori_loop(0, count, one, 0)

    def slot_of(dy, same):
        return (zl if same else 1 - zl) * 4 + at_y(dy)

    send("jz+", j(0, 0), "z+")
    send("jz-", j(0, 0), "z-")
    ring_send("y", A0, True)
    ring_send("y", A1, True)
    x_send(0)
    send("zA0", i(A0, 0), "zi")
    ring_send("y", V, True)
    for copy in small:
        copy.wait()
    loop(2, inverse_rows)

    x_forward(0)
    ring_got("y", A0, True, "+")
    ring_forward("y", A0, True, "+")
    got("jz+", j(0, -1))
    got("jz-", j(0, 1))
    send("jzf+", j(0, -1, 0, 2), "z+")
    send("jzf-", j(0, 1, 2, 4), "z-")
    x_send(-1)
    x_send(1)
    send("zA1", i(A1, 0), "zi")
    send("zU", i(U, 0), "zi")
    send("zV.0", i(V, 0), "zi")
    ring_got("y", A1, True, "-")
    ring_forward("y", A1, True, "-")
    loop(2, lambda n: inverse_rows(n + 2))
    got("zA0", i(A0, 0, False))
    ring_send("p", A0, False)
    ring_got("y", V, True, "+")
    ring_got("y", V, True, "-")
    send("zV.-", i(V, -1), "zi")
    send("zV.+", i(V, 1), "zi")
    ring_forward("y", VP["+"], True, "+")
    ring_forward("y", VP["-"], True, "-")
    loop(2, lambda n: inverse_rows(n + 4))
    got("jzf+", j(0, 2, 0, 2))
    got("jzf-", j(0, 2, 2, 4))
    x_send(2)
    x_forward(-1)
    x_forward(1)
    x_got_forward(0)
    share(0)
    loop(2, lambda n: inverse_rows(n + 6))
    got("zA1", i(A1, 0, False))
    ring_send("p", A1, False)
    ring_got("p", A0, False, "+")
    ring_forward("p", A0, False, "+")
    x_forward(2)
    ring_got_forward("y", VP["+"], True, "+")
    ring_got_forward("y", VP["-"], True, "-")
    send("zV.2", i(V, 2), "zi")
    ring_got("p", A1, False, "-")
    ring_forward("p", A1, False, "-")
    ring_send("y", U, True)
    got("zU", i(U, 0, False))
    ring_send("p", U, False)
    x_got_forward(-1)
    x_got_forward(1)
    for dx in (-1, 1):
        share(dx)
    x_got_forward(2)
    share(2)
    for dx in (0, -1, 1, 2):
        got_share(dx)
    loop(8, mix_right)
    mirror_slots([(0, True)], first=True)
    ring_got("y", A0, True, "-")
    ring_got("y", A1, True, "+")
    ring_got_forward("y", A0, True, "+")
    ring_got_forward("y", A1, True, "-")
    ring_got("p", A0, False, "-")
    ring_got("p", A1, False, "+")
    ring_got_forward("p", A0, False, "+")
    ring_got_forward("p", A1, False, "-")
    loop(8, mix_left)
    direct_tile(0)
    ring_got("y", U, True, "+")
    ring_forward("y", UP["+"], True, "+")
    ring_got("y", U, True, "-")
    ring_forward("y", UP["-"], True, "-")
    direct_tile(1)
    ring_got("p", U, False, "+")
    ring_forward("p", UP["+"], False, "+")
    ring_got("p", U, False, "-")
    ring_forward("p", UP["-"], False, "-")
    got("zV.0", i(V, 0, False))
    mirror_slots([(-1, True), (1, True), (0, False)])
    got("zV.-", i(V, -1, False))
    got("zV.+", i(V, 1, False))
    load.wait()
    ring_got_forward("y", UP["+"], True, "+")
    ring_got_forward("y", UP["-"], True, "-")
    mirror_slots([(-1, False), (1, False), (2, True)], last=True)
    for copy in sent[:-6]:
        copy.wait_send()
    got("zV.2", i(V, 2, False))
    ring_got_forward("p", UP["+"], False, "+")
    ring_got_forward("p", UP["-"], False, "-")
    turn(0, slot_of(2, False))
    for copy in sent[-6:]:
        copy.wait_send()
    assert len(ids) <= N_MSG


def finish_kernel(base, inv, wt, rmt, result, stage, sem):
    col = lax.axis_index("col")
    slot = (1 - col // 4) * 4 + lax.rem(col + 2, 4)
    copies = []
    for m in range(4):
        rows = slice(m * 256, m * 256 + 256)
        total = jnp.dot(wt[rows, :256], rmt[slot], preferred_element_type=F32)
        stage[rows] = base[rows] + total * inv[rows]
        copies.append(pltpu.make_async_copy(stage.at[rows], result.at[rows], sem.at[m]))
        copies[-1].start()
    for copy in copies:
        copy.wait()


def body(amplitudes, panels_left, panels_right, weights_right, weights_left, energy_left, energy_right, energy_virtual):
    middle = pl.pallas_call(
        gather_kernel,
        out_shape=[
            jax.ShapeDtypeStruct((1024, 1024), F32),
            jax.ShapeDtypeStruct((1024, 1024), F32),
            jax.ShapeDtypeStruct((1024, 768), BF16),
            jax.ShapeDtypeStruct((8, 256, 1024), BF16),
        ],
        in_specs=[pl.BlockSpec(memory_space=pltpu.HBM)] * 6 + [pl.BlockSpec(memory_space=pltpu.SMEM)] * 2,
        out_specs=[pl.BlockSpec(memory_space=pltpu.VMEM)] * 4,
        scratch_shapes=[
            pltpu.VMEM((8, 512, 1024), BF16),
            pltpu.VMEM((4, 4, 4, 2, 32, 1024), BF16),
            pltpu.VMEM((2, 1024, 1024), BF16),
            pltpu.VMEM((1024, 1024), F32),
            pltpu.VMEM((8, 128), F32),
            pltpu.SemaphoreType.DMA((6,)),
            pltpu.SemaphoreType.DMA((N_MSG,)),
            pltpu.SemaphoreType.DMA((N_MSG,)),
        ],
        compiler_params=pltpu.CompilerParams(
            collective_id=0, has_side_effects=True, vmem_limit_bytes=36 * 1024 * 1024
        ),
        name="gather_products",
    )(*(pltpu.with_memory_space_constraint(array, pltpu.HBM) for array in (
        panels_left.reshape(256, 1024), panels_right[0], weights_right[:, 0], weights_left.reshape(256, 1024),
        amplitudes[0, 0],
        energy_virtual.reshape(8, 128))), energy_left, energy_right)
    updated = pl.pallas_call(
        finish_kernel,
        out_shape=jax.ShapeDtypeStruct((1024, 1024), F32),
        in_specs=[pl.BlockSpec(memory_space=pltpu.VMEM)] * 4,
        out_specs=pl.BlockSpec(memory_space=pltpu.HBM),
        scratch_shapes=[pltpu.VMEM((1024, 1024), F32), pltpu.SemaphoreType.DMA((4,))],
        compiler_params=pltpu.CompilerParams(vmem_limit_bytes=12 * 1024 * 1024),
        name="finish",
    )(*middle)
    return updated[None, None]


def solution(mesh):
    placed = (
        P("row", "col", None, None),
        P("row", None, "col", None),
        P("col", None, "row", None),
        P(None, "col", "row", None),
        P(None, "row", "col", None),
        P("row"),
        P("col"),
        P(),
    )
    return jax.shard_map(
        body, mesh=mesh, in_specs=placed, out_specs=P("row", "col", None, None), check_vma=False
    )
```

```python
import jax
import jax.numpy as jnp
from jax import lax
from jax.experimental import pallas as pl
from jax.experimental.pallas import tpu as pltpu
from jax.sharding import PartitionSpec as P

MESH = pl.DeviceIdType.MESH
F32 = jnp.float32
BF16 = jnp.bfloat16
N_MSG = 56
BLOCKS = ((0, 256), (256, 256), (512, 256), (768, 256))
CUT = 112


def gather_kernel(panl, panr, wtr, wtl, amp_in, ev_in, el, er, out, inv, wt, rmt, awi, awj, lm, amp, ev,
                  lsem, ssem, rsem):
    row, col = lax.axis_index("row"), lax.axis_index("col")
    x, zh, core = row // 8, lax.rem(row // 2, 4), lax.rem(row, 2)
    zl, y = col // 4, lax.rem(col, 4)

    def at_x(d):
        return lax.rem(x + d + 4, 4)

    def at_z(d):
        return lax.rem(zh + d + 4, 4)

    def at_y(d):
        return lax.rem(y + d + 4, 4)

    def row_of(x_, zh_, core_):
        return (x_ * 4 + zh_) * 2 + core_

    dev = {
        "x+": (row_of(at_x(1), zh, core), col),
        "x-": (row_of(at_x(-1), zh, core), col),
        "z+": (row_of(x, at_z(1), core), col),
        "z-": (row_of(x, at_z(-1), core), col),
        "y+": (row, zl * 4 + at_y(1)),
        "y-": (row, zl * 4 + at_y(-1)),
        "zi": (row, (1 - zl) * 4 + y),
        "core": (row_of(x, zh, 1 - core), col),
    }

    own = [
        pltpu.make_async_copy(panl, awi.at[col, 0:256], lsem.at[0]),
        pltpu.make_async_copy(panr, awj.at[0:2, x, zh, core], lsem.at[1]),
        pltpu.make_async_copy(wtr, awj.at[2:4, x, zh, core], lsem.at[2]),
        pltpu.make_async_copy(wtl, awi.at[col, 256:512], lsem.at[3]),
    ]
    small = [
        pltpu.make_async_copy(ev_in, ev, lsem.at[4]),
    ]
    load = pltpu.make_async_copy(amp_in, amp, lsem.at[5])
    for copy in (own[1], own[2], own[0], own[3], *small):
        copy.start()

    barrier = pltpu.get_barrier_semaphore()
    for peer in dev.values():
        pl.semaphore_signal(barrier, inc=1, device_id=peer, device_id_type=MESH)
    pl.semaphore_wait(barrier, len(dev))

    ids = {}
    sent = []

    def describe(name, ref, to):
        number = ids.setdefault(name, len(ids))
        return pltpu.make_async_remote_copy(
            src_ref=ref, dst_ref=ref, send_sem=ssem.at[number], recv_sem=rsem.at[number],
            device_id=dev[to], device_id_type=MESH,
        )

    def send(name, ref, to):
        copy = describe(name, ref, to)
        copy.start()
        sent.append(copy)

    def got(name, ref):
        describe(name, ref, "core").wait_recv()

    def j(dx, dz, lo=0, hi=4):
        return awj.at[lo:hi, at_x(dx), at_z(dz), core]

    def i(part, dy, same=True):
        return awi.at[(zl if same else 1 - zl) * 4 + at_y(dy), part[0]:part[1]]

    A0, A1, U, V = (0, 128), (128, 256), (256, 256 + CUT), (256 + CUT, 512)
    UP = {"+": (256, 320), "-": (320, 256 + CUT)}
    VP = {"+": (256 + CUT, 320 + CUT), "-": (320 + CUT, 464), "late": (464, 512)}
    STEP = {"+": 1, "-": -1}

    def ring_send(tag, part, same):
        for s in "+-":
            send(f"{tag}{part}{s}", i(part, 0, same), "y" + s)

    def ring_got(tag, part, same, s):
        got(f"{tag}{part}{s}", i(part, -STEP[s], same))

    def ring_forward(tag, part, same, s):
        send(f"{tag}f{part}{s}", i(part, -STEP[s], same), "y" + s)

    def ring_got_forward(tag, part, same, s):
        got(f"{tag}f{part}{s}", i(part, 2, same))

    def x_send(dz):
        for s in "+-":
            send(f"x{dz}{s}", j(0, dz), "x" + s)

    def x_forward(dz):
        for s in "+-":
            got(f"x{dz}{s}", j(-STEP[s], dz))
        send(f"xf{dz}+", j(-1, dz, 0, 2), "x+")
        send(f"xf{dz}-", j(1, dz, 2, 4), "x-")

    def x_got_forward(dz):
        got(f"xf{dz}+", j(2, dz, 0, 2))
        got(f"xf{dz}-", j(2, dz, 2, 4))

    def share(dx):
        send(f"core{dx}", awj.at[:, at_x(dx), :, core], "core")

    def got_share(dx):
        got(f"core{dx}", awj.at[:, at_x(dx), :, 1 - core])

    def mix_left(k, blk):
        start = pl.multiple_of(blk * 128, 128)
        own_rows = slice(k * 128, k * 128 + 128)
        for h in range(2):
            cols = slice(h * 512, h * 512 + 512)
            straight = awi[blk, own_rows, cols]
            turned = awi[h * 4:h * 4 + 4, own_rows, pl.ds(start, 128)].reshape(512, 128).T
            lm[k, pl.ds(start, 128), cols] = straight + straight - turned

    def mix_right(blk):
        start = pl.multiple_of(blk * 128, 128)

        def one(k, _):
            for h in range(2):
                cols = slice(h * 512, h * 512 + 512)
                straight = awj[k, blk // 2, pl.ds(lax.rem(blk, 2) * 2, 2), :, :, cols].reshape(128, 512)
                turned = awj[k, h * 2:h * 2 + 2, :, :, :, pl.ds(start, 128)].reshape(512, 128).T
                rmt[blk, pl.ds(pl.multiple_of(k * 128, 128), 128), cols] = turned + turned - straight
            return _

        lax.fori_loop(0, 2, one, 0)

    def direct_tile(n):
        cols = pl.ds(pl.multiple_of(n * 512, 512), 512)
        total = jnp.dot(lm[0], awj[2, :, :, :, :, cols].reshape(1024, 512), preferred_element_type=F32)
        total += jnp.dot(lm[1], awj[3, :, :, :, :, cols].reshape(1024, 512), preferred_element_type=F32)
        out[:, cols] += total

    def turn(p, slot):
        for k in range(2):
            for h in range(2):
                cols = slice(h * 512, h * 512 + 512)
                start = (2 * p + k) * 128
                wt[cols, start:start + 128] = awi[slot, 256 + k * 128:384 + k * 128, cols].T

    def mirror_slots(places, first=False, last=False):
        slots = [slot_of(*place) for place in places]
        for p, slot in enumerate(slots):
            turn(p, slot)

        def one(n, _):
            cols = pl.ds(pl.multiple_of(n * 512, 512), 512)
            total = jnp.zeros((1024, 512), F32) if first else out[:, cols]
            for p, slot in enumerate(slots):
                total += jnp.dot(wt[:, p * 256:p * 256 + 256], rmt[slot, :, cols], preferred_element_type=F32)
            out[:, cols] = amp[:, cols] + total * inv[:, cols] if last else total
            return _

        lax.fori_loop(0, 2, one, 0)

    def inverse_rows(blk):
        pair = el[0] + er[0]
        turned = jnp.broadcast_to(ev[pl.ds(blk, 1), :], (128, 128)).T
        for q in range(8):
            virt_pair = turned + ev[q:q + 1, :]
            inv[pl.ds(pl.multiple_of(blk * 128, 128), 128), q * 128:q * 128 + 128] = 1.0 / (pair - virt_pair)

    def loop(count, task):
        def one(n, _):
            task(n)
            return _
        lax.fori_loop(0, count, one, 0)

    def slot_of(dy, same):
        return (zl if same else 1 - zl) * 4 + at_y(dy)

    own[1].wait()
    own[2].wait()
    send("jz+", j(0, 0), "z+")
    send("jz-", j(0, 0), "z-")
    own[0].wait()
    ring_send("y", A0, True)
    ring_send("y", A1, True)
    x_send(0)
    send("zA0", i(A0, 0), "zi")
    own[3].wait()
    ring_send("y", V, True)
    load.start()
    for copy in small:
        copy.wait()
    loop(2, inverse_rows)

    x_forward(0)
    ring_got("y", A0, True, "+")
    ring_forward("y", A0, True, "+")
    got("jz+", j(0, -1))
    got("jz-", j(0, 1))
    send("jzf+", j(0, -1, 0, 2), "z+")
    send("jzf-", j(0, 1, 2, 4), "z-")
    x_send(-1)
    x_send(1)
    send("zA1", i(A1, 0), "zi")
    send("zU", i(U, 0), "zi")
    send("zV.0", i(V, 0), "zi")
    ring_got("y", A1, True, "-")
    ring_forward("y", A1, True, "-")
    loop(2, lambda n: inverse_rows(n + 2))
    got("zA0", i(A0, 0, False))
    ring_send("p", A0, False)
    ring_got("y", V, True, "+")
    ring_got("y", V, True, "-")
    send("zV.-", i(V, -1), "zi")
    send("zV.+", i(V, 1), "zi")
    ring_forward("y", VP["+"], True, "+")
    ring_forward("y", VP["-"], True, "-")
    loop(2, lambda n: inverse_rows(n + 4))
    got("jzf+", j(0, 2, 0, 2))
    got("jzf-", j(0, 2, 2, 4))
    x_send(2)
    x_forward(-1)
    x_forward(1)
    x_got_forward(0)
    share(0)
    loop(2, lambda n: inverse_rows(n + 6))
    got("zA1", i(A1, 0, False))
    ring_send("p", A1, False)
    ring_forward("y", VP["late"], True, "-")
    ring_got("p", A0, False, "+")
    ring_forward("p", A0, False, "+")
    x_forward(2)
    ring_got("p", A1, False, "-")
    ring_forward("p", A1, False, "-")
    ring_send("y", U, True)
    ring_got_forward("y", VP["+"], True, "+")
    ring_got_forward("y", VP["-"], True, "-")
    ring_got_forward("y", VP["late"], True, "-")
    send("zV.2", i(V, 2), "zi")
    got("zU", i(U, 0, False))
    ring_send("p", U, False)
    x_got_forward(-1)
    x_got_forward(1)
    for dx in (-1, 1):
        share(dx)
    x_got_forward(2)
    share(2)
    for dx in (0, -1, 1, 2):
        got_share(dx)
    loop(8, mix_right)
    mirror_slots([(0, True)], first=True)
    ring_got("y", A0, True, "-")
    ring_got_forward("y", A0, True, "+")
    ring_got("p", A0, False, "-")
    ring_got_forward("p", A0, False, "+")
    loop(8, lambda n: mix_left(0, n))
    ring_got("y", A1, True, "+")
    ring_got_forward("y", A1, True, "-")
    ring_got("p", A1, False, "+")
    ring_got_forward("p", A1, False, "-")
    loop(8, lambda n: mix_left(1, n))
    direct_tile(0)
    ring_got("y", U, True, "+")
    ring_forward("y", UP["+"], True, "+")
    ring_got("y", U, True, "-")
    ring_forward("y", UP["-"], True, "-")
    direct_tile(1)
    ring_got("p", U, False, "+")
    ring_forward("p", UP["+"], False, "+")
    ring_got("p", U, False, "-")
    ring_forward("p", UP["-"], False, "-")
    got("zV.0", i(V, 0, False))
    mirror_slots([(-1, True), (1, True), (0, False)])
    got("zV.-", i(V, -1, False))
    got("zV.+", i(V, 1, False))
    load.wait()
    ring_got_forward("y", UP["+"], True, "+")
    ring_got_forward("y", UP["-"], True, "-")
    mirror_slots([(-1, False), (1, False), (2, True)], last=True)
    for copy in sent[:-6]:
        copy.wait_send()
    got("zV.2", i(V, 2, False))
    ring_got_forward("p", UP["+"], False, "+")
    ring_got_forward("p", UP["-"], False, "-")
    turn(0, slot_of(2, False))
    for copy in sent[-6:]:
        copy.wait_send()
    assert len(ids) <= N_MSG


def finish_kernel(base, inv, wt, rmt, result, stage, sem):
    col = lax.axis_index("col")
    slot = (1 - col // 4) * 4 + lax.rem(col + 2, 4)
    copies = []
    for m, (start, size) in enumerate(BLOCKS):
        rows = slice(start, start + size)
        total = jnp.dot(wt[rows, :256], rmt[slot], preferred_element_type=F32)
        stage[rows] = base[rows] + total * inv[rows]
        copies.append(pltpu.make_async_copy(stage.at[rows], result.at[rows], sem.at[m]))
        copies[-1].start()
    for copy in copies:
        copy.wait()


def body(amplitudes, panels_left, panels_right, weights_right, weights_left, energy_left, energy_right, energy_virtual):
    middle = pl.pallas_call(
        gather_kernel,
        out_shape=[
            jax.ShapeDtypeStruct((1024, 1024), F32),
            jax.ShapeDtypeStruct((1024, 1024), F32),
            jax.ShapeDtypeStruct((1024, 768), BF16),
            jax.ShapeDtypeStruct((8, 256, 1024), BF16),
        ],
        in_specs=[pl.BlockSpec(memory_space=pltpu.HBM)] * 6 + [pl.BlockSpec(memory_space=pltpu.SMEM)] * 2,
        out_specs=[pl.BlockSpec(memory_space=pltpu.VMEM)] * 4,
        scratch_shapes=[
            pltpu.VMEM((8, 512, 1024), BF16),
            pltpu.VMEM((4, 4, 4, 2, 32, 1024), BF16),
            pltpu.VMEM((2, 1024, 1024), BF16),
            pltpu.VMEM((1024, 1024), F32),
            pltpu.VMEM((8, 128), F32),
            pltpu.SemaphoreType.DMA((6,)),
            pltpu.SemaphoreType.DMA((N_MSG,)),
            pltpu.SemaphoreType.DMA((N_MSG,)),
        ],
        compiler_params=pltpu.CompilerParams(
            collective_id=0, has_side_effects=True, vmem_limit_bytes=36 * 1024 * 1024
        ),
        name="gather_products",
    )(*(pltpu.with_memory_space_constraint(array, pltpu.HBM) for array in (
        panels_left.reshape(256, 1024), panels_right[0], weights_right[:, 0], weights_left.reshape(256, 1024),
        amplitudes[0, 0],
        energy_virtual.reshape(8, 128))), energy_left, energy_right)
    updated = pl.pallas_call(
        finish_kernel,
        out_shape=jax.ShapeDtypeStruct((1024, 1024), F32),
        in_specs=[pl.BlockSpec(memory_space=pltpu.VMEM)] * 4,
        out_specs=pl.BlockSpec(memory_space=pltpu.HBM),
        scratch_shapes=[pltpu.VMEM((1024, 1024), F32), pltpu.SemaphoreType.DMA((len(BLOCKS),))],
        compiler_params=pltpu.CompilerParams(vmem_limit_bytes=12 * 1024 * 1024),
        name="finish",
    )(*middle)
    return updated[None, None]


def solution(mesh):
    placed = (
        P("row", "col", None, None),
        P("row", None, "col", None),
        P("col", None, "row", None),
        P(None, "col", "row", None),
        P(None, "row", "col", None),
        P("row"),
        P("col"),
        P(),
    )
    return jax.shard_map(
        body, mesh=mesh, in_specs=placed, out_specs=P("row", "col", None, None), check_vma=False
    )
```

```python
import jax
import jax.numpy as jnp
from jax import lax
from jax.experimental import pallas as pl
from jax.experimental.pallas import tpu as pltpu
from jax.sharding import PartitionSpec as P

MESH = pl.DeviceIdType.MESH
F32 = jnp.float32
BF16 = jnp.bfloat16
N_MSG = 56
BLOCKS = ((0, 256), (256, 256), (512, 256), (768, 256))
CUT = 112


def gather_kernel(panl, panr, wtr, wtl, amp_in, ev_in, el, er, out, inv, wt, rmt, awi, awj, lm, amp, ev,
                  lsem, ssem, rsem):
    row, col = lax.axis_index("row"), lax.axis_index("col")
    x, zh, core = row // 8, lax.rem(row // 2, 4), lax.rem(row, 2)
    zl, y = col // 4, lax.rem(col, 4)

    def at_x(d):
        return lax.rem(x + d + 4, 4)

    def at_z(d):
        return lax.rem(zh + d + 4, 4)

    def at_y(d):
        return lax.rem(y + d + 4, 4)

    def row_of(x_, zh_, core_):
        return (x_ * 4 + zh_) * 2 + core_

    dev = {
        "x+": (row_of(at_x(1), zh, core), col),
        "x-": (row_of(at_x(-1), zh, core), col),
        "z+": (row_of(x, at_z(1), core), col),
        "z-": (row_of(x, at_z(-1), core), col),
        "y+": (row, zl * 4 + at_y(1)),
        "y-": (row, zl * 4 + at_y(-1)),
        "zi": (row, (1 - zl) * 4 + y),
        "core": (row_of(x, zh, 1 - core), col),
    }

    own = [
        pltpu.make_async_copy(panl, awi.at[col, 0:256], lsem.at[0]),
        pltpu.make_async_copy(panr, awj.at[0:2, x, zh, core], lsem.at[1]),
        pltpu.make_async_copy(wtr, awj.at[2:4, x, zh, core], lsem.at[2]),
        pltpu.make_async_copy(wtl, awi.at[col, 256:512], lsem.at[3]),
    ]
    small = [
        pltpu.make_async_copy(ev_in, ev, lsem.at[4]),
    ]
    load = pltpu.make_async_copy(amp_in, amp, lsem.at[5])
    for copy in (own[1], own[2], own[0], own[3], *small):
        copy.start()

    barrier = pltpu.get_barrier_semaphore()
    for peer in dev.values():
        pl.semaphore_signal(barrier, inc=1, device_id=peer, device_id_type=MESH)
    pl.semaphore_wait(barrier, len(dev))

    ids = {}
    sent = []

    def describe(name, ref, to):
        number = ids.setdefault(name, len(ids))
        return pltpu.make_async_remote_copy(
            src_ref=ref, dst_ref=ref, send_sem=ssem.at[number], recv_sem=rsem.at[number],
            device_id=dev[to], device_id_type=MESH,
        )

    def send(name, ref, to):
        copy = describe(name, ref, to)
        copy.start()
        sent.append(copy)

    def got(name, ref):
        describe(name, ref, "core").wait_recv()

    def j(dx, dz, lo=0, hi=4):
        return awj.at[lo:hi, at_x(dx), at_z(dz), core]

    def i(part, dy, same=True):
        return awi.at[(zl if same else 1 - zl) * 4 + at_y(dy), part[0]:part[1]]

    A0, A1, U, V = (0, 128), (128, 256), (256, 256 + CUT), (256 + CUT, 512)
    UP = {"+": (256, 320), "-": (320, 256 + CUT)}
    VP = {"+": (256 + CUT, 320 + CUT), "-": (320 + CUT, 464), "late": (464, 512)}
    STEP = {"+": 1, "-": -1}

    def ring_send(tag, part, same):
        for s in "+-":
            send(f"{tag}{part}{s}", i(part, 0, same), "y" + s)

    def ring_got(tag, part, same, s):
        got(f"{tag}{part}{s}", i(part, -STEP[s], same))

    def ring_forward(tag, part, same, s):
        send(f"{tag}f{part}{s}", i(part, -STEP[s], same), "y" + s)

    def ring_got_forward(tag, part, same, s):
        got(f"{tag}f{part}{s}", i(part, 2, same))

    def x_send(dz):
        for s in "+-":
            send(f"x{dz}{s}", j(0, dz), "x" + s)

    def x_forward(dz):
        for s in "+-":
            got(f"x{dz}{s}", j(-STEP[s], dz))
        send(f"xf{dz}+", j(-1, dz, 0, 2), "x+")
        send(f"xf{dz}-", j(1, dz, 2, 4), "x-")

    def x_got_forward(dz):
        got(f"xf{dz}+", j(2, dz, 0, 2))
        got(f"xf{dz}-", j(2, dz, 2, 4))

    def share(dx):
        send(f"core{dx}", awj.at[:, at_x(dx), :, core], "core")

    def got_share(dx):
        got(f"core{dx}", awj.at[:, at_x(dx), :, 1 - core])

    def mix_left(k, blk):
        start = pl.multiple_of(blk * 128, 128)
        own_rows = slice(k * 128, k * 128 + 128)
        for h in range(2):
            cols = slice(h * 512, h * 512 + 512)
            straight = awi[blk, own_rows, cols]
            turned = awi[h * 4:h * 4 + 4, own_rows, pl.ds(start, 128)].reshape(512, 128).T
            lm[k, pl.ds(start, 128), cols] = straight + straight - turned

    def mix_right(d1, d2):
        g1, g2 = at_x(d1), at_x(d2)
        cols = pl.ds(pl.multiple_of(g2 * 256, 256), 256)
        for k in range(2):
            for half in range(2):
                blk = g1 * 2 + half
                turned = awj[k, g2, :, :, :, pl.ds(pl.multiple_of(blk * 128, 128), 128)].reshape(256, 128).T
                straight = awj[k, g1, 2 * half:2 * half + 2, :, :, cols].reshape(128, 256)
                rmt[blk, k * 128:k * 128 + 128, cols] = turned + turned - straight

    def direct_tile(n):
        cols = pl.ds(pl.multiple_of(n * 512, 512), 512)
        total = jnp.dot(lm[0], awj[2, :, :, :, :, cols].reshape(1024, 512), preferred_element_type=F32)
        total += jnp.dot(lm[1], awj[3, :, :, :, :, cols].reshape(1024, 512), preferred_element_type=F32)
        out[:, cols] += total

    def turn(p, slot):
        for k in range(2):
            for h in range(2):
                cols = slice(h * 512, h * 512 + 512)
                start = (2 * p + k) * 128
                wt[cols, start:start + 128] = awi[slot, 256 + k * 128:384 + k * 128, cols].T

    def mirror_slots(places, first=False, last=False):
        slots = [slot_of(*place) for place in places]
        for p, slot in enumerate(slots):
            turn(p, slot)

        def one(n, _):
            cols = pl.ds(pl.multiple_of(n * 512, 512), 512)
            total = jnp.zeros((1024, 512), F32) if first else out[:, cols]
            for p, slot in enumerate(slots):
                total += jnp.dot(wt[:, p * 256:p * 256 + 256], rmt[slot, :, cols], preferred_element_type=F32)
            out[:, cols] = amp[:, cols] + total * inv[:, cols] if last else total
            return _

        lax.fori_loop(0, 2, one, 0)

    def inverse_rows(blk):
        pair = el[0] + er[0]
        turned = jnp.broadcast_to(ev[pl.ds(blk, 1), :], (128, 128)).T
        for q in range(8):
            virt_pair = turned + ev[q:q + 1, :]
            inv[pl.ds(pl.multiple_of(blk * 128, 128), 128), q * 128:q * 128 + 128] = 1.0 / (pair - virt_pair)

    def loop(count, task):
        def one(n, _):
            task(n)
            return _
        lax.fori_loop(0, count, one, 0)

    def slot_of(dy, same):
        return (zl if same else 1 - zl) * 4 + at_y(dy)

    own[1].wait()
    own[2].wait()
    send("jz+", j(0, 0), "z+")
    send("jz-", j(0, 0), "z-")
    own[0].wait()
    ring_send("y", A0, True)
    ring_send("y", A1, True)
    x_send(0)
    send("zA0", i(A0, 0), "zi")
    own[3].wait()
    ring_send("y", V, True)
    load.start()
    for copy in small:
        copy.wait()
    loop(2, inverse_rows)

    x_forward(0)
    ring_got("y", A0, True, "+")
    ring_forward("y", A0, True, "+")
    got("jz+", j(0, -1))
    got("jz-", j(0, 1))
    send("jzf+", j(0, -1, 0, 2), "z+")
    send("jzf-", j(0, 1, 2, 4), "z-")
    x_send(-1)
    x_send(1)
    send("zA1", i(A1, 0), "zi")
    send("zU", i(U, 0), "zi")
    send("zV.0", i(V, 0), "zi")
    ring_got("y", A1, True, "-")
    ring_forward("y", A1, True, "-")
    loop(2, lambda n: inverse_rows(n + 2))
    got("zA0", i(A0, 0, False))
    ring_send("p", A0, False)
    ring_got("y", V, True, "+")
    ring_got("y", V, True, "-")
    send("zV.-", i(V, -1), "zi")
    send("zV.+", i(V, 1), "zi")
    ring_forward("y", VP["+"], True, "+")
    ring_forward("y", VP["-"], True, "-")
    loop(2, lambda n: inverse_rows(n + 4))
    got("jzf+", j(0, 2, 0, 2))
    got("jzf-", j(0, 2, 2, 4))
    x_send(2)
    x_forward(-1)
    x_forward(1)
    x_got_forward(0)
    share(0)
    loop(2, lambda n: inverse_rows(n + 6))
    got("zA1", i(A1, 0, False))
    ring_send("p", A1, False)
    ring_forward("y", VP["late"], True, "-")
    ring_got("p", A0, False, "+")
    ring_forward("p", A0, False, "+")
    x_forward(2)
    ring_got("p", A1, False, "-")
    ring_forward("p", A1, False, "-")
    ring_send("y", U, True)
    ring_got_forward("y", VP["+"], True, "+")
    ring_got_forward("y", VP["-"], True, "-")
    ring_got_forward("y", VP["late"], True, "-")
    send("zV.2", i(V, 2), "zi")
    got("zU", i(U, 0, False))
    ring_send("p", U, False)
    for dx in (-1, 1):
        share(dx)
    for dx in (0, -1, 1):
        got_share(dx)
    loop(9, lambda n: mix_right(n // 3 - 1, lax.rem(n, 3) - 1))
    x_got_forward(-1)
    x_got_forward(1)
    x_got_forward(2)
    share(2)
    got_share(2)
    loop(4, lambda n: mix_right(2, n - 1))
    loop(3, lambda n: mix_right(n - 1, 2))
    mirror_slots([(0, True)], first=True)
    ring_got("y", A0, True, "-")
    ring_got_forward("y", A0, True, "+")
    ring_got("p", A0, False, "-")
    ring_got_forward("p", A0, False, "+")
    loop(8, lambda n: mix_left(0, n))
    ring_got("y", A1, True, "+")
    ring_got_forward("y", A1, True, "-")
    ring_got("p", A1, False, "+")
    ring_got_forward("p", A1, False, "-")
    loop(8, lambda n: mix_left(1, n))
    direct_tile(0)
    ring_got("y", U, True, "+")
    ring_forward("y", UP["+"], True, "+")
    ring_got("y", U, True, "-")
    ring_forward("y", UP["-"], True, "-")
    direct_tile(1)
    ring_got("p", U, False, "+")
    ring_forward("p", UP["+"], False, "+")
    ring_got("p", U, False, "-")
    ring_forward("p", UP["-"], False, "-")
    got("zV.0", i(V, 0, False))
    mirror_slots([(-1, True), (1, True), (0, False)])
    got("zV.-", i(V, -1, False))
    got("zV.+", i(V, 1, False))
    load.wait()
    ring_got_forward("y", UP["+"], True, "+")
    ring_got_forward("y", UP["-"], True, "-")
    mirror_slots([(-1, False), (1, False), (2, True)], last=True)
    for copy in sent[:-6]:
        copy.wait_send()
    got("zV.2", i(V, 2, False))
    ring_got_forward("p", UP["+"], False, "+")
    ring_got_forward("p", UP["-"], False, "-")
    turn(0, slot_of(2, False))
    for copy in sent[-6:]:
        copy.wait_send()
    assert len(ids) <= N_MSG


def finish_kernel(base, inv, wt, rmt, result, stage, sem):
    col = lax.axis_index("col")
    slot = (1 - col // 4) * 4 + lax.rem(col + 2, 4)
    copies = []
    for m, (start, size) in enumerate(BLOCKS):
        rows = slice(start, start + size)
        total = jnp.dot(wt[rows, :256], rmt[slot], preferred_element_type=F32)
        stage[rows] = base[rows] + total * inv[rows]
        copies.append(pltpu.make_async_copy(stage.at[rows], result.at[rows], sem.at[m]))
        copies[-1].start()
    for copy in copies:
        copy.wait()


def body(amplitudes, panels_left, panels_right, weights_right, weights_left, energy_left, energy_right, energy_virtual):
    middle = pl.pallas_call(
        gather_kernel,
        out_shape=[
            jax.ShapeDtypeStruct((1024, 1024), F32),
            jax.ShapeDtypeStruct((1024, 1024), F32),
            jax.ShapeDtypeStruct((1024, 768), BF16),
            jax.ShapeDtypeStruct((8, 256, 1024), BF16),
        ],
        in_specs=[pl.BlockSpec(memory_space=pltpu.HBM)] * 6 + [pl.BlockSpec(memory_space=pltpu.SMEM)] * 2,
        out_specs=[pl.BlockSpec(memory_space=pltpu.VMEM)] * 4,
        scratch_shapes=[
            pltpu.VMEM((8, 512, 1024), BF16),
            pltpu.VMEM((4, 4, 4, 2, 32, 1024), BF16),
            pltpu.VMEM((2, 1024, 1024), BF16),
            pltpu.VMEM((1024, 1024), F32),
            pltpu.VMEM((8, 128), F32),
            pltpu.SemaphoreType.DMA((6,)),
            pltpu.SemaphoreType.DMA((N_MSG,)),
            pltpu.SemaphoreType.DMA((N_MSG,)),
        ],
        compiler_params=pltpu.CompilerParams(
            collective_id=0, has_side_effects=True, vmem_limit_bytes=36 * 1024 * 1024
        ),
        name="gather_products",
    )(*(pltpu.with_memory_space_constraint(array, pltpu.HBM) for array in (
        panels_left.reshape(256, 1024), panels_right[0], weights_right[:, 0], weights_left.reshape(256, 1024),
        amplitudes[0, 0],
        energy_virtual.reshape(8, 128))), energy_left, energy_right)
    updated = pl.pallas_call(
        finish_kernel,
        out_shape=jax.ShapeDtypeStruct((1024, 1024), F32),
        in_specs=[pl.BlockSpec(memory_space=pltpu.VMEM)] * 4,
        out_specs=pl.BlockSpec(memory_space=pltpu.HBM),
        scratch_shapes=[pltpu.VMEM((1024, 1024), F32), pltpu.SemaphoreType.DMA((len(BLOCKS),))],
        compiler_params=pltpu.CompilerParams(vmem_limit_bytes=12 * 1024 * 1024),
        name="finish",
    )(*middle)
    return updated[None, None]


def solution(mesh):
    placed = (
        P("row", "col", None, None),
        P("row", None, "col", None),
        P("col", None, "row", None),
        P(None, "col", "row", None),
        P(None, "row", "col", None),
        P("row"),
        P("col"),
        P(),
    )
    return jax.shard_map(
        body, mesh=mesh, in_specs=placed, out_specs=P("row", "col", None, None), check_vma=False
    )
```

```python
import jax
import jax.numpy as jnp
from jax import lax
from jax.experimental import pallas as pl
from jax.experimental.pallas import tpu as pltpu
from jax.sharding import PartitionSpec as P

MESH = pl.DeviceIdType.MESH
F32 = jnp.float32
BF16 = jnp.bfloat16
N_MSG = 56
BLOCKS = ((0, 256), (256, 256), (512, 256), (768, 256))
CUT = 112


def gather_kernel(panl, panr, wtr, wtl, amp_in, ev_in, el, er, out, inv, wt, rmt, awi, awj, lm, amp, ev,
                  lsem, ssem, rsem):
    row, col = lax.axis_index("row"), lax.axis_index("col")
    x, zh, core = row // 8, lax.rem(row // 2, 4), lax.rem(row, 2)
    zl, y = col // 4, lax.rem(col, 4)

    def at_x(d):
        return lax.rem(x + d + 4, 4)

    def at_z(d):
        return lax.rem(zh + d + 4, 4)

    def at_y(d):
        return lax.rem(y + d + 4, 4)

    def row_of(x_, zh_, core_):
        return (x_ * 4 + zh_) * 2 + core_

    dev = {
        "x+": (row_of(at_x(1), zh, core), col),
        "x-": (row_of(at_x(-1), zh, core), col),
        "z+": (row_of(x, at_z(1), core), col),
        "z-": (row_of(x, at_z(-1), core), col),
        "y+": (row, zl * 4 + at_y(1)),
        "y-": (row, zl * 4 + at_y(-1)),
        "zi": (row, (1 - zl) * 4 + y),
        "core": (row_of(x, zh, 1 - core), col),
    }

    own = [
        pltpu.make_async_copy(panl, awi.at[col, 0:256], lsem.at[0]),
        pltpu.make_async_copy(panr, awj.at[0:2, x, zh, core], lsem.at[1]),
        pltpu.make_async_copy(wtr, awj.at[2:4, x, zh, core], lsem.at[2]),
        pltpu.make_async_copy(wtl, awi.at[col, 256:512], lsem.at[3]),
    ]
    small = [
        pltpu.make_async_copy(ev_in, ev, lsem.at[4]),
    ]
    load = pltpu.make_async_copy(amp_in, amp, lsem.at[5])
    for copy in (own[1], own[2], own[0], own[3], *small):
        copy.start()

    barrier = pltpu.get_barrier_semaphore()
    for peer in dev.values():
        pl.semaphore_signal(barrier, inc=1, device_id=peer, device_id_type=MESH)
    pl.semaphore_wait(barrier, len(dev))

    ids = {}
    sent = []

    def describe(name, ref, to):
        number = ids.setdefault(name, len(ids))
        return pltpu.make_async_remote_copy(
            src_ref=ref, dst_ref=ref, send_sem=ssem.at[number], recv_sem=rsem.at[number],
            device_id=dev[to], device_id_type=MESH,
        )

    def send(name, ref, to):
        copy = describe(name, ref, to)
        copy.start()
        sent.append(copy)

    def got(name, ref):
        describe(name, ref, "core").wait_recv()

    def j(dx, dz, lo=0, hi=4):
        return awj.at[lo:hi, at_x(dx), at_z(dz), core]

    def i(part, dy, same=True):
        return awi.at[(zl if same else 1 - zl) * 4 + at_y(dy), part[0]:part[1]]

    A0, A1, U, V = (0, 128), (128, 256), (256, 256 + CUT), (256 + CUT, 512)
    UP = {"+": (256, 320), "-": (320, 256 + CUT)}
    VP = {"+": (256 + CUT, 320 + CUT), "-": (320 + CUT, 464), "late": (464, 512)}
    STEP = {"+": 1, "-": -1}

    def ring_send(tag, part, same):
        for s in "+-":
            send(f"{tag}{part}{s}", i(part, 0, same), "y" + s)

    def ring_got(tag, part, same, s):
        got(f"{tag}{part}{s}", i(part, -STEP[s], same))

    def ring_forward(tag, part, same, s):
        send(f"{tag}f{part}{s}", i(part, -STEP[s], same), "y" + s)

    def ring_got_forward(tag, part, same, s):
        got(f"{tag}f{part}{s}", i(part, 2, same))

    def x_send(dz):
        for s in "+-":
            send(f"x{dz}{s}", j(0, dz), "x" + s)

    def x_forward(dz):
        for s in "+-":
            got(f"x{dz}{s}", j(-STEP[s], dz))
        send(f"xf{dz}+", j(-1, dz, 0, 2), "x+")
        send(f"xf{dz}-", j(1, dz, 2, 4), "x-")

    def x_got_forward(dz):
        got(f"xf{dz}+", j(2, dz, 0, 2))
        got(f"xf{dz}-", j(2, dz, 2, 4))

    def share(dx):
        send(f"core{dx}", awj.at[:, at_x(dx), :, core], "core")

    def got_share(dx):
        got(f"core{dx}", awj.at[:, at_x(dx), :, 1 - core])

    def mix_left(k, blk):
        start = pl.multiple_of(blk * 128, 128)
        own_rows = slice(k * 128, k * 128 + 128)
        for h in range(2):
            cols = slice(h * 512, h * 512 + 512)
            straight = awi[blk, own_rows, cols]
            turned = awi[h * 4:h * 4 + 4, own_rows, pl.ds(start, 128)].reshape(512, 128).T
            lm[k, pl.ds(start, 128), cols] = straight + straight - turned

    def mix_right(d1, d2):
        g1, g2 = at_x(d1), at_x(d2)
        cols = pl.ds(pl.multiple_of(g2 * 256, 256), 256)
        for k in range(2):
            for half in range(2):
                blk = g1 * 2 + half
                turned = awj[k, g2, :, :, :, pl.ds(pl.multiple_of(blk * 128, 128), 128)].reshape(256, 128).T
                straight = awj[k, g1, 2 * half:2 * half + 2, :, :, cols].reshape(128, 256)
                rmt[blk, k * 128:k * 128 + 128, cols] = turned + turned - straight

    def direct_tile(n):
        cols = pl.ds(pl.multiple_of(n * 512, 512), 512)
        total = jnp.dot(lm[0], awj[2, :, :, :, :, cols].reshape(1024, 512), preferred_element_type=F32)
        total += jnp.dot(lm[1], awj[3, :, :, :, :, cols].reshape(1024, 512), preferred_element_type=F32)
        out[:, cols] += total

    def turn(p, slot):
        for k in range(2):
            for h in range(2):
                cols = slice(h * 512, h * 512 + 512)
                start = (2 * p + k) * 128
                wt[cols, start:start + 128] = awi[slot, 256 + k * 128:384 + k * 128, cols].T

    def mirror_slots(places, first=False, last=False):
        slots = [slot_of(*place) for place in places]
        for p, slot in enumerate(slots):
            turn(p, slot)

        def one(n, _):
            cols = pl.ds(pl.multiple_of(n * 512, 512), 512)
            total = jnp.zeros((1024, 512), F32) if first else out[:, cols]
            for p, slot in enumerate(slots):
                total += jnp.dot(wt[:, p * 256:p * 256 + 256], rmt[slot, :, cols], preferred_element_type=F32)
            out[:, cols] = amp[:, cols] + total * inv[:, cols] if last else total
            return _

        lax.fori_loop(0, 2, one, 0)

    def inverse_rows(blk):
        pair = el[0] + er[0]
        turned = jnp.broadcast_to(ev[pl.ds(blk, 1), :], (128, 128)).T
        for q in range(8):
            virt_pair = turned + ev[q:q + 1, :]
            inv[pl.ds(pl.multiple_of(blk * 128, 128), 128), q * 128:q * 128 + 128] = 1.0 / (pair - virt_pair)

    def loop(count, task):
        def one(n, _):
            task(n)
            return _
        lax.fori_loop(0, count, one, 0)

    def slot_of(dy, same):
        return (zl if same else 1 - zl) * 4 + at_y(dy)

    own[1].wait()
    own[2].wait()
    send("jz+", j(0, 0), "z+")
    send("jz-", j(0, 0), "z-")
    own[0].wait()
    ring_send("y", A0, True)
    ring_send("y", A1, True)
    x_send(0)
    send("zA0", i(A0, 0), "zi")
    own[3].wait()
    ring_send("y", V, True)
    load.start()
    for copy in small:
        copy.wait()
    loop(2, inverse_rows)

    x_forward(0)
    ring_got("y", A0, True, "+")
    ring_forward("y", A0, True, "+")
    got("jz+", j(0, -1))
    got("jz-", j(0, 1))
    send("jzf+", j(0, -1, 0, 2), "z+")
    send("jzf-", j(0, 1, 2, 4), "z-")
    x_send(-1)
    x_send(1)
    send("zA1", i(A1, 0), "zi")
    send("zU", i(U, 0), "zi")
    send("zV.0", i(V, 0), "zi")
    ring_got("y", A1, True, "-")
    ring_forward("y", A1, True, "-")
    loop(2, lambda n: inverse_rows(n + 2))
    got("zA0", i(A0, 0, False))
    ring_send("p", A0, False)
    ring_got("y", V, True, "+")
    ring_got("y", V, True, "-")
    send("zV.-", i(V, -1), "zi")
    send("zV.+", i(V, 1), "zi")
    ring_forward("y", VP["+"], True, "+")
    ring_forward("y", VP["-"], True, "-")
    loop(2, lambda n: inverse_rows(n + 4))
    got("jzf+", j(0, 2, 0, 2))
    got("jzf-", j(0, 2, 2, 4))
    x_send(2)
    x_forward(-1)
    x_forward(1)
    x_got_forward(0)
    share(0)
    loop(2, lambda n: inverse_rows(n + 6))
    got("zA1", i(A1, 0, False))
    ring_send("p", A1, False)
    ring_forward("y", VP["late"], True, "-")
    ring_got("p", A0, False, "+")
    ring_forward("p", A0, False, "+")
    x_forward(2)
    ring_got("p", A1, False, "-")
    ring_forward("p", A1, False, "-")
    ring_send("y", U, True)
    ring_got_forward("y", VP["+"], True, "+")
    ring_got_forward("y", VP["-"], True, "-")
    ring_got_forward("y", VP["late"], True, "-")
    send("zV.2", i(V, 2), "zi")
    got("zU", i(U, 0, False))
    ring_send("p", U, False)
    for dx in (-1, 1):
        share(dx)
    for dx in (0, -1, 1):
        got_share(dx)
    loop(9, lambda n: mix_right(n // 3 - 1, lax.rem(n, 3) - 1))
    x_got_forward(-1)
    x_got_forward(1)
    x_got_forward(2)
    share(2)
    ring_got("y", A0, True, "-")
    ring_got_forward("y", A0, True, "+")
    ring_got("p", A0, False, "-")
    ring_got_forward("p", A0, False, "+")
    loop(8, lambda n: mix_left(0, n))
    got_share(2)
    loop(4, lambda n: mix_right(2, n - 1))
    loop(3, lambda n: mix_right(n - 1, 2))
    mirror_slots([(0, True)], first=True)
    ring_got("y", A1, True, "+")
    ring_got_forward("y", A1, True, "-")
    ring_got("p", A1, False, "+")
    ring_got_forward("p", A1, False, "-")
    loop(8, lambda n: mix_left(1, n))
    direct_tile(0)
    ring_got("y", U, True, "+")
    ring_forward("y", UP["+"], True, "+")
    ring_got("y", U, True, "-")
    ring_forward("y", UP["-"], True, "-")
    direct_tile(1)
    ring_got("p", U, False, "+")
    ring_forward("p", UP["+"], False, "+")
    ring_got("p", U, False, "-")
    ring_forward("p", UP["-"], False, "-")
    got("zV.0", i(V, 0, False))
    mirror_slots([(-1, True), (1, True), (0, False)])
    got("zV.-", i(V, -1, False))
    got("zV.+", i(V, 1, False))
    load.wait()
    ring_got_forward("y", UP["+"], True, "+")
    ring_got_forward("y", UP["-"], True, "-")
    mirror_slots([(-1, False), (1, False), (2, True)], last=True)
    for copy in sent[:-6]:
        copy.wait_send()
    got("zV.2", i(V, 2, False))
    ring_got_forward("p", UP["+"], False, "+")
    ring_got_forward("p", UP["-"], False, "-")
    turn(0, slot_of(2, False))
    for copy in sent[-6:]:
        copy.wait_send()
    assert len(ids) <= N_MSG


def finish_kernel(base, inv, wt, rmt, result, stage, sem):
    col = lax.axis_index("col")
    slot = (1 - col // 4) * 4 + lax.rem(col + 2, 4)
    copies = []
    for m, (start, size) in enumerate(BLOCKS):
        rows = slice(start, start + size)
        total = jnp.dot(wt[rows, :256], rmt[slot], preferred_element_type=F32)
        stage[rows] = base[rows] + total * inv[rows]
        copies.append(pltpu.make_async_copy(stage.at[rows], result.at[rows], sem.at[m]))
        copies[-1].start()
    for copy in copies:
        copy.wait()


def body(amplitudes, panels_left, panels_right, weights_right, weights_left, energy_left, energy_right, energy_virtual):
    middle = pl.pallas_call(
        gather_kernel,
        out_shape=[
            jax.ShapeDtypeStruct((1024, 1024), F32),
            jax.ShapeDtypeStruct((1024, 1024), F32),
            jax.ShapeDtypeStruct((1024, 768), BF16),
            jax.ShapeDtypeStruct((8, 256, 1024), BF16),
        ],
        in_specs=[pl.BlockSpec(memory_space=pltpu.HBM)] * 6 + [pl.BlockSpec(memory_space=pltpu.SMEM)] * 2,
        out_specs=[pl.BlockSpec(memory_space=pltpu.VMEM)] * 4,
        scratch_shapes=[
            pltpu.VMEM((8, 512, 1024), BF16),
            pltpu.VMEM((4, 4, 4, 2, 32, 1024), BF16),
            pltpu.VMEM((2, 1024, 1024), BF16),
            pltpu.VMEM((1024, 1024), F32),
            pltpu.VMEM((8, 128), F32),
            pltpu.SemaphoreType.DMA((6,)),
            pltpu.SemaphoreType.DMA((N_MSG,)),
            pltpu.SemaphoreType.DMA((N_MSG,)),
        ],
        compiler_params=pltpu.CompilerParams(
            collective_id=0, has_side_effects=True, vmem_limit_bytes=36 * 1024 * 1024
        ),
        name="gather_products",
    )(*(pltpu.with_memory_space_constraint(array, pltpu.HBM) for array in (
        panels_left.reshape(256, 1024), panels_right[0], weights_right[:, 0], weights_left.reshape(256, 1024),
        amplitudes[0, 0],
        energy_virtual.reshape(8, 128))), energy_left, energy_right)
    updated = pl.pallas_call(
        finish_kernel,
        out_shape=jax.ShapeDtypeStruct((1024, 1024), F32),
        in_specs=[pl.BlockSpec(memory_space=pltpu.VMEM)] * 4,
        out_specs=pl.BlockSpec(memory_space=pltpu.HBM),
        scratch_shapes=[pltpu.VMEM((1024, 1024), F32), pltpu.SemaphoreType.DMA((len(BLOCKS),))],
        compiler_params=pltpu.CompilerParams(vmem_limit_bytes=12 * 1024 * 1024),
        name="finish",
    )(*middle)
    return updated[None, None]


def solution(mesh):
    placed = (
        P("row", "col", None, None),
        P("row", None, "col", None),
        P("col", None, "row", None),
        P(None, "col", "row", None),
        P(None, "row", "col", None),
        P("row"),
        P("col"),
        P(),
    )
    return jax.shard_map(
        body, mesh=mesh, in_specs=placed, out_specs=P("row", "col", None, None), check_vma=False
    )
```
